32 devices in a mesh: groups: 2 (over x), section: 2 (over core), mesh: 8 (over z, y).
Axes of the slice: x: 2, y: 2, z: 4, core: 2. Of those that a mesh axis runs over, the one named last changes fastest.
Arguments:
- inputs: bfloat16 [4, 128, 8192], P('groups', None, 'mesh'), parts along dimension 0, may hold values from -12 to 12
- segments: int32 [4, 128], P('groups'), parts along dimension 0, may hold values from 0 to 3, never falling along the last dimension, each value on 1 to 64 neighbouring positions
- gains: bfloat16 [2, 1, 8192], P('section'), may hold values from 0.25 to 1.75
- w_query: bfloat16 [2, 1, 8192, 1024], P('section', None, None, 'mesh'), may hold values from -1.3258252 to 1.3258252
- w_keyval: bfloat16 [2, 1, 8192, 256], P('section', None, None, 'mesh'), may hold values from -0.055242717 to 0.055242717
- w_output: bfloat16 [2, 1, 1024, 8192], P('section', None, None, 'mesh'), may hold values from -0.1875 to 0.1875
Outputs:
- section_outputs: bfloat16 [2, 4, 128, 8192], P('section', 'groups', None, 'mesh'), parts along dimension 1
The draws below stay inside these ranges and needn't reach their ends.
There are 2 independent parts, one for each index of `groups`. The reference program is written for one: setup_inputs(seed, part) draws one part's arguments, and reference() takes and returns one part's arrays. A program takes and returns all parts, laid end to end along the dimension named above; an argument that names none is the same for every part. Nothing has to cross between parts.
Inputs may be any that keep to these rules, and one draw needn't show every extreme that they name: `segments`: along each micro-batch the document ids never fall; each document spans 1 to 64 positions.
All inputs are finite; a program needn't handle non-finite values.
Results may differ from the reference program's by a relative error of at most 0.0052.
Values may be sent and summed in bfloat16 or wider, within the bound.
A program may use at most 64 MiB of HBM per device.

```python
import math
import jax
import jax.numpy as jnp
import numpy as np
from jax import lax

D = 8192
HD = 128
GROUP = 8
TOK = 128
MICRO = 2
LAYERS = 1
HEADS = 8
KVH = 1
SECTIONS = 2
SEGS = 4


def keyval_base(key):
    shape_kv = (SECTIONS, LAYERS, D, KVH * 2 * HD)
    base = jax.random.normal(jax.random.fold_in(key, 11), shape_kv, jnp.float32)
    return jnp.clip(base, -5.0, 5.0) / math.sqrt(D)


def draw_w_keyval(key, part):
    return keyval_base(key).astype(jnp.bfloat16)


def draw_w_query(key, part):
    value = jnp.clip(jax.random.normal(jax.random.fold_in(key, 19), (SECTIONS, LAYERS, D, HEADS, HD), jnp.float32), -5.0, 5.0) / math.sqrt(D)
    return value.reshape(SECTIONS, LAYERS, D, HEADS * HD).astype(jnp.bfloat16)


def draw_inputs(key, part):
    columns = jnp.arange(D, dtype=jnp.int32).astype(jnp.float32)
    rising = jnp.sqrt(1.0 + 2.0 * columns / D)
    rough = jnp.exp(jax.random.uniform(jax.random.fold_in(key, 3), (D,), jnp.float32, math.log(0.7), math.log(1.4)))
    base = jax.random.normal(jax.random.fold_in(key, 5), (MICRO, TOK, D), jnp.float32)
    value = base
    return jnp.clip(value * rising * rough, -12.0, 12.0).astype(jnp.bfloat16)


def levels(own_key, dims, shards, smallest, high):
    def one(dim, parts):
        steps = jax.random.uniform(jax.random.fold_in(jax.random.fold_in(own_key, 6), dim), (parts,), jnp.float32, smallest / len(shards), high / len(shards))
        return jnp.repeat(jnp.exp(steps), dims[dim] // parts).reshape((-1,) + (1,) * (len(dims) - dim - 1))

    loudness = one(*shards[0])
    for cut in shards[1:]:
        loudness = loudness * one(*cut)
    return loudness


def profile(number_of, total, limit, lean):
    loads = [(1 << 20) // math.isqrt(rank ** lean) + 1 for rank in range(2, number_of + 1)]
    rest, given = total - limit - (number_of - 1), [1] * (number_of - 1)
    while rest > 0:
        movable = [i for i in range(number_of - 1) if given[i] < limit]
        mass, left = sum([loads[i] for i in movable]), rest
        for i in movable:
            extra = min(limit - given[i], max(1, left * loads[i] // mass), rest)
            given[i] = given[i] + extra
            rest = rest - extra
    return np.array([limit] + given)


def uneven_parts(rng, number_of, total, reach, slope):
    if number_of == 2:
        one = jax.random.randint(rng, (), max(1, total - reach), min(reach, total - 1) + 1)
        return jnp.stack([one, total - one])
    lengths = jnp.asarray(profile(number_of, total, reach, slope), jnp.int32)
    pairs = (number_of - 1) // 2
    donor, taker = lengths[1:1 + 2 * pairs:2], lengths[2:2 + 2 * pairs:2]
    slack = jnp.minimum(donor - 1, reach - taker)
    moved = jax.random.randint(jax.random.fold_in(rng, 1), (pairs,), 0, 1 << 20) % (slack + 1)
    lengths = lengths.at[1:1 + 2 * pairs:2].set(donor - moved).at[2:2 + 2 * pairs:2].set(taker + moved)
    return lengths[jax.random.permutation(jax.random.fold_in(rng, 2), number_of)]


def bell_draw(stream_key, shape, scale, limit, shards=(), kind=jnp.bfloat16):
    drawn = jax.random.normal(stream_key, shape, jnp.float32) * scale
    if len(shards) > 0:
        drawn = levels(stream_key, shape, shards, -0.22, 0.18) * drawn
    return jnp.clip(drawn, min=-limit, max=limit).astype(kind)


def setup_inputs(seed: int = 0, part: int = 0) -> dict:
    seeds = jax.random.split(jax.random.key(seed), 7)
    own_keys = jax.random.split(jax.random.fold_in(seeds[6], part), 7)
    return {
        "inputs": draw_inputs(jax.random.fold_in(jax.random.fold_in(seeds[6], part), 71), part),
        "segments": jax.vmap(lambda own: jnp.searchsorted(jnp.cumsum(uneven_parts(own, SEGS, TOK, TOK // 2, 1)), jnp.arange(TOK), side="right"))(jax.random.split(own_keys[1], MICRO)).reshape((MICRO, TOK)).astype(jnp.int32),
        "gains": jnp.clip(1.0 + 0.15 * jax.random.normal(seeds[2], (SECTIONS, LAYERS, D), jnp.float32), 0.25, 1.75).astype(jnp.bfloat16),
        "w_query": draw_w_query(jax.random.fold_in(seeds[6], 71), part),
        "w_keyval": draw_w_keyval(jax.random.fold_in(seeds[6], 71), part),
        "w_output": bell_draw(seeds[5], (SECTIONS, LAYERS, HEADS * HD, D), (HEADS * HD) ** -0.5, 0.1875, ((0, 2), (3, 8))),
    }


norm_epsilon = 1e-05
rope_theta = 500000.0

def position_tables(segment_row):
    row_length = segment_row.shape[0]
    indices = jnp.arange(row_length, dtype=jnp.int32)
    doc_starts = jnp.concatenate([jnp.ones((1,), dtype=bool), segment_row[1:] != segment_row[:-1]])
    first_index = lax.cummax(jnp.where(doc_starts, indices, jnp.zeros_like(indices)), axis=0)
    positions = (indices - first_index).astype(jnp.float32)
    half_width = HD // 2
    freqs = rope_theta ** (-(2.0 * jnp.arange(half_width, dtype=jnp.float32)) / HD)
    angles = positions[:, None] * freqs[None, :]
    cosine_table = jnp.concatenate([jnp.cos(angles), jnp.cos(angles)], axis=1)
    sine_table = jnp.concatenate([jnp.sin(angles), jnp.sin(angles)], axis=1)
    allowed = (indices[None, :] <= indices[:, None]) & (segment_row[None, :] == segment_row[:, None])
    return (cosine_table, sine_table, allowed)

def rotate(values, cosine_table, sine_table):
    half_width = values.shape[-1] // 2
    turned = jnp.concatenate([-values[..., half_width:], values[..., :half_width]], axis=-1)
    return values * cosine_table + turned * sine_table

def softmax_weights(scores, allowed):
    masked = jnp.where(allowed, scores, -1e+30)
    highest = lax.optimization_barrier(jnp.max(masked, axis=-1, keepdims=True))
    raised = jnp.exp(masked - highest)
    return (raised / lax.optimization_barrier(jnp.sum(raised, axis=-1, keepdims=True))).astype(jnp.bfloat16)

def apply_layer(activations, gain_row, query_weight, keyval_weight, output_weight, tables):
    cosine_table, sine_table, allowed = tables
    floats = activations.astype(jnp.float32)
    row_count = floats.shape[0]
    scale = lax.rsqrt(lax.optimization_barrier(jnp.mean(floats * floats, axis=1, keepdims=True)) + norm_epsilon)
    normed = (floats * scale * gain_row.astype(jnp.float32)).astype(jnp.bfloat16)
    query = jnp.dot(normed, query_weight, preferred_element_type=jnp.float32).reshape(row_count, HEADS, HD)
    query = rotate(query, cosine_table[:, None, :], sine_table[:, None, :]).astype(jnp.bfloat16)
    keyval = jnp.dot(normed, keyval_weight, preferred_element_type=jnp.float32).astype(jnp.bfloat16)
    keyval = keyval.reshape(row_count, KVH, 2, HD)
    keys = rotate(keyval[:, :, 0, :].astype(jnp.float32), cosine_table[:, None, :], sine_table[:, None, :]).astype(jnp.bfloat16)
    values = keyval[:, :, 1, :]
    grouped = query.reshape(row_count, KVH, GROUP, HD)
    scores = jnp.einsum('tgqd,sgd->gqts', grouped.astype(jnp.float32), keys.astype(jnp.float32)) * HD ** (-0.5)
    probs = softmax_weights(scores, allowed[None, None, :, :])
    attended = jnp.einsum('gqts,sgd->tgqd', probs.astype(jnp.float32), values.astype(jnp.float32))
    attended = attended.astype(jnp.bfloat16).reshape(row_count, HEADS * HD)
    mixed = jnp.dot(attended, output_weight, preferred_element_type=jnp.float32)
    return (floats + mixed).astype(jnp.bfloat16)

def reference(inputs, segments, gains, w_query, w_keyval, w_output):
    tables = [position_tables(segments[micro_index]) for micro_index in range(MICRO)]
    current = [inputs[micro_index] for micro_index in range(MICRO)]
    results = []
    for section_index in range(SECTIONS):
        for micro_index in range(MICRO):
            for layer_index in range(LAYERS):
                current[micro_index] = apply_layer(current[micro_index], gains[section_index, layer_index], w_query[section_index, layer_index], w_keyval[section_index, layer_index], w_output[section_index, layer_index], tables[micro_index])
        results.append(jnp.stack(current))
    return jnp.stack(results)
```

```python
import functools
import math

import jax
import jax.numpy as jnp
import numpy as np
from jax import lax
from jax.experimental import pallas as pl
from jax.experimental.pallas import tpu as pltpu
from jax.sharding import PartitionSpec as P

HD = 128
GROUP = 8
norm_epsilon = 1e-05
rope_theta = 500000.0
MESH = pl.DeviceIdType.MESH
F32 = jnp.float32
BF16 = jnp.bfloat16


def inner_of(n):
    inner = 1
    while inner * 2 * inner * 2 <= n:
        inner *= 2
    return inner


def kernel(
    n,
    x_hbm,
    seg_ref,
    freq_ref,
    g_hbm,
    wq_hbm,
    wkv_hbm,
    wo_hbm,
    out_ref,
    xbuf,
    wq,
    wkv,
    wo,
    gbuf,
    ssq,
    kvbuf,
    att,
    fin,
    acc,
    scale_ref,
    cos_ref,
    sin_ref,
    mask_ref,
    in_sem,
    w_sem,
    w_send,
    x_recv,
    z_send,
    y_send,
    ssq_recv,
    ssq_send,
    kv_recv,
    kv_send,
    att_recv,
    att_send,
    out_send,
    out_recv,
    out_local,
):
    core = lax.axis_index("section")
    me = lax.axis_index("mesh")
    other = 1 - core
    inner = inner_of(n)
    outer = n // inner
    row, lane = me // inner, me % inner
    tok, cols = x_hbm.shape[1:]
    width = n * cols
    kvw = wkv_hbm.shape[1]
    first = me // GROUP * GROUP

    def block(layer, src):
        return xbuf.at[layer, :, pl.ds(pl.multiple_of(src * cols, cols), cols)]

    def send_to(src, dst, send, recv, peer):
        return pltpu.make_async_remote_copy(
            src_ref=src, dst_ref=dst, send_sem=send, recv_sem=recv,
            device_id={"mesh": peer}, device_id_type=MESH,
        )

    load_x = pltpu.make_async_copy(x_hbm.at[core], block(0, me), in_sem)
    load_x.start()
    weights = ((g_hbm, gbuf), (wq_hbm, wq), (wkv_hbm, wkv), (wo_hbm, wo))
    own_weights = [
        pltpu.make_async_copy(src, dst.at[core], w_sem.at[core, k]) for k, (src, dst) in enumerate(weights)
    ]
    sent_weights = [
        pltpu.make_async_remote_copy(
            src_ref=src, dst_ref=dst.at[core], send_sem=w_send.at[k], recv_sem=w_sem.at[core, k],
            device_id={"section": other}, device_id_type=MESH,
        )
        for k, (src, dst) in enumerate(weights)
    ]
    for copy in own_weights:
        copy.start()

    barrier = pltpu.get_barrier_semaphore()

    def greet(k, carry):
        pl.semaphore_signal(barrier, inc=1, device_id={"mesh": (me + k) % n}, device_id_type=MESH)
        return carry

    lax.fori_loop(1, n, greet, 0)
    pl.semaphore_signal(barrier, inc=1, device_id={"section": other}, device_id_type=MESH)
    load_x.wait()
    pl.semaphore_wait(barrier, n)

    def z_copy(layer, src, sign):
        return send_to(
            block(layer, src), block(layer, src), z_send.at[layer, (sign + 1) // 2, src // inner],
            x_recv.at[layer, src], me + sign * inner,
        )

    def y_copy(layer, src, k):
        return send_to(
            block(layer, src), block(layer, src), y_send.at[layer, k, src // inner],
            x_recv.at[layer, src], row * inner + (lane + k) % inner,
        )

    def arrived(layer, src):
        y_copy(layer, src, 0).wait_recv()

    def over_y(body):
        if inner == 2:
            body(1)
        else:
            def step(k, carry):
                body(k)
                return carry
            lax.fori_loop(1, inner, step, 0)

    def forward(layer, src, signs):
        for sign in signs:
            @pl.when((row + sign >= 0) & (row + sign < outer))
            def _():
                z_copy(layer, src, sign).start()
        over_y(lambda k: y_copy(layer, src, k).start())

    def over_peers(total, base, mine, body):
        def step(k, carry):
            body(base + (mine - base + k) % total)
            return carry
        lax.fori_loop(1, total, step, 0)

    def ssq_copy(layer, peer):
        return send_to(ssq.at[layer, me], ssq.at[layer, me], ssq_send.at[layer, peer], ssq_recv.at[layer, me], peer)

    def ssq_wait(layer, peer):
        send_to(ssq.at[layer, peer], ssq.at[layer, peer], ssq_send.at[layer, peer], ssq_recv.at[layer, peer], peer).wait_recv()

    def send_own(layer, value):
        floats = value.astype(F32)
        total = jnp.sum(floats * floats, axis=1, keepdims=True)
        ssq[layer, me] = jnp.transpose(jnp.broadcast_to(total, (tok, tok)))[:8]
        over_peers(n, 0, me, lambda peer: ssq_copy(layer, peer).start())
        forward(layer, me, (1, -1))

    send_own(0, block(0, me)[...])
    for copy in sent_weights:
        copy.start()

    seg = jnp.broadcast_to(seg_ref[pl.ds(core, 1), :].astype(F32), (tok, tok))
    t_index = lax.broadcasted_iota(jnp.int32, (tok, tok), 0)
    u_index = lax.broadcasted_iota(jnp.int32, (tok, tok), 1)
    allowed = jnp.where((seg == jnp.transpose(seg)) & (u_index <= t_index), 1.0, 0.0)
    mask_ref[...] = allowed
    positions = jnp.sum(allowed, axis=1, keepdims=True) - 1.0
    angles = positions * freq_ref[0:1, :]
    cos_ref[...] = jnp.cos(angles)
    sine = jnp.sin(angles)
    head_lane = lax.broadcasted_iota(jnp.int32, (tok, HD), 1)
    sin_ref[...] = jnp.where(head_lane < HD // 2, -sine, sine)

    def rope(values):
        return (values * cos_ref[...] + pltpu.roll(values, HD // 2, 1) * sin_ref[...]).astype(BF16)

    def weight_wait(layer, k):
        src, dst = weights[k]
        pltpu.make_async_copy(src, dst.at[layer], w_sem.at[layer, k]).wait()

    def consume(layer, src):
        span = pl.ds(pl.multiple_of(src * cols, cols), cols)
        scale = jnp.concatenate([scale_ref[...]] * (cols // HD), axis=1)
        normed = (xbuf[layer, :, span].astype(F32) * scale * gbuf[layer, :, span].astype(F32)).astype(BF16)
        both = jnp.concatenate([wq[layer, span, :], wkv[layer, span, :]], axis=1)
        acc[...] += jnp.dot(normed, both, preferred_element_type=F32)

    for layer in range(2):
        over_peers(n, 0, me, lambda peer: ssq_wait(layer, peer))
        total = jnp.sum(ssq[layer], axis=0)
        scale_ref[...] = jnp.transpose(
            jnp.broadcast_to(lax.rsqrt(total[0:1, :] * (1.0 / width) + norm_epsilon), (HD, tok))
        )
        for k in range(3):
            weight_wait(layer, k)
        acc[...] = jnp.zeros_like(acc)
        consume(layer, me)

        def side_blocks(distance):
            for sign in (1, -1):
                src_row = row - sign * distance

                @pl.when((src_row >= 0) & (src_row < outer))
                def _():
                    def take(k):
                        src = src_row * inner + (lane + k) % inner
                        arrived(layer, src)
                        consume(layer, src)
                    over_y(take)

        def wave(distance, carry):
            for sign in (1, -1):
                src_row = row - sign * distance

                @pl.when((src_row >= 0) & (src_row < outer))
                def _():
                    src = src_row * inner + lane
                    arrived(layer, src)
                    forward(layer, src, (sign,))
                    consume(layer, src)

            @pl.when(distance > 1)
            def _():
                side_blocks(distance - 1)
            return carry

        def take_own_row(k):
            src = row * inner + (lane + k) % inner
            arrived(layer, src)
            consume(layer, src)

        lax.fori_loop(1, 2, wave, 0)
        over_y(take_own_row)
        lax.fori_loop(2, outer, wave, 0)
        side_blocks(outer - 1)

        kvbuf[layer, me - first] = acc[:, HD:].astype(BF16)

        def kv_copy(peer):
            return send_to(
                kvbuf.at[layer, me - first], kvbuf.at[layer, me - first],
                kv_send.at[layer, peer - first], kv_recv.at[layer, me - first], peer,
            )

        def kv_wait(peer):
            send_to(
                kvbuf.at[layer, peer - first], kvbuf.at[layer, peer - first],
                kv_send.at[layer, peer - first], kv_recv.at[layer, peer - first], peer,
            ).wait_recv()

        over_peers(GROUP, first, me, lambda peer: kv_copy(peer).start())
        query = rope(acc[:, :HD])
        over_peers(GROUP, first, me, kv_wait)
        keyval = jnp.concatenate([kvbuf[layer, j] for j in range(GROUP)], axis=1)
        keys = rope(keyval[:, :HD].astype(F32))
        scores = lax.dot_general(
            query, keys, (((1,), (1,)), ((), ())), preferred_element_type=F32
        ) * HD ** (-0.5)
        masked = jnp.where(mask_ref[...] > 0.0, scores, -1e30)
        raised = jnp.exp(masked - jnp.max(masked, axis=1, keepdims=True))
        probs = (raised / jnp.sum(raised, axis=1, keepdims=True)).astype(BF16)
        attended = jnp.dot(probs, keyval[:, HD:], preferred_element_type=F32).astype(BF16)

        def att_block(src):
            return att.at[layer, :, pl.ds(pl.multiple_of(src * HD, HD), HD)]

        def att_copy(peer):
            return send_to(att_block(me), att_block(me), att_send.at[layer, peer], att_recv.at[layer, me], peer)

        def att_wait(peer):
            send_to(att_block(peer), att_block(peer), att_send.at[layer, peer], att_recv.at[layer, peer], peer).wait_recv()

        att_block(me)[...] = attended
        over_peers(n, 0, me, lambda peer: att_copy(peer).start())
        weight_wait(layer, 3)
        over_peers(n, 0, me, att_wait)
        mixed = jnp.dot(att[layer], wo[layer], preferred_element_type=F32)
        result = (block(layer, me)[...].astype(F32) + mixed).astype(BF16)
        if layer == 0:
            block(1, me)[...] = result
            send_own(1, result)
            kept = block(1, me)
        else:
            fin[...] = result
            kept = fin

        @pl.when(core == layer)
        def _():
            pltpu.make_async_copy(kept, out_ref.at[core], out_local).start()

        @pl.when(core != layer)
        def _():
            pltpu.make_async_remote_copy(
                src_ref=kept, dst_ref=out_ref.at[core], send_sem=out_send, recv_sem=out_recv,
                device_id={"section": other}, device_id_type=MESH,
            ).start()

        over_peers(GROUP, first, me, lambda peer: kv_copy(peer).wait_send())
        over_peers(n, 0, me, lambda peer: att_copy(peer).wait_send())

    for layer in range(2):
        over_peers(n, 0, me, lambda peer: ssq_copy(layer, peer).wait_send())

        def drain(src_row, carry):
            src = src_row * inner + lane

            @pl.when((src_row <= row) & (row + 1 < outer))
            def _():
                z_copy(layer, src, 1).wait_send()

            @pl.when((src_row >= row) & (row >= 1))
            def _():
                z_copy(layer, src, -1).wait_send()

            over_y(lambda k: y_copy(layer, src, k).wait_send())
            return carry

        lax.fori_loop(0, outer, drain, 0)
    for copy in sent_weights:
        copy.wait_send()
    pltpu.make_async_copy(fin, out_ref.at[core], out_local).wait()
    last = pltpu.make_async_remote_copy(
        src_ref=fin, dst_ref=out_ref.at[other], send_sem=out_send, recv_sem=out_recv,
        device_id={"section": other}, device_id_type=MESH,
    )
    last.wait_send()
    last.wait_recv()


def shards(n, inputs, segments, gains, w_query, w_keyval, w_output):
    micro_count, tok, cols = inputs.shape
    width = gains.shape[-1]
    kvw = w_keyval.shape[-1]
    inner = inner_of(n)
    outer = n // inner
    half = HD // 2
    freqs = np.float32(rope_theta) ** (-(2.0 * np.arange(half, dtype=np.float32)) / np.float32(HD))
    freqs = np.broadcast_to(np.concatenate([freqs, freqs])[None].astype(np.float32), (8, HD))
    dma = pltpu.SemaphoreType.DMA
    vmem = pl.BlockSpec(memory_space=pltpu.VMEM)
    hbm = pl.BlockSpec(memory_space=pl.ANY)
    out = pl.pallas_call(
        functools.partial(kernel, n),
        out_shape=jax.ShapeDtypeStruct((micro_count, tok, cols), BF16),
        in_specs=[hbm, vmem, vmem, hbm, hbm, hbm, hbm],
        out_specs=hbm,
        scratch_shapes=[
            pltpu.VMEM((2, tok, width), BF16),
            pltpu.VMEM((2, width, HD), BF16),
            pltpu.VMEM((2, width, kvw), BF16),
            pltpu.VMEM((2,) + w_output.shape[2:], BF16),
            pltpu.VMEM((2, 1, width), BF16),
            pltpu.VMEM((2, n, 8, tok), F32),
            pltpu.VMEM((2, GROUP, tok, kvw), BF16),
            pltpu.VMEM((2, tok, n * HD), BF16),
            pltpu.VMEM((tok, cols), BF16),
            pltpu.VMEM((tok, HD + kvw), F32),
            pltpu.VMEM((tok, HD), F32),
            pltpu.VMEM((tok, HD), F32),
            pltpu.VMEM((tok, HD), F32),
            pltpu.VMEM((tok, tok), F32),
            dma,
            dma((2, 4)),
            dma((4,)),
            dma((2, n)),
            dma((2, 2, outer)),
            dma((2, max(inner, 2), outer)),
            dma((2, n)),
            dma((2, n)),
            dma((2, GROUP)),
            dma((2, GROUP)),
            dma((2, n)),
            dma((2, n)),
            dma,
            dma,
            dma,
        ],
        compiler_params=pltpu.CompilerParams(
            collective_id=0, has_side_effects=True, vmem_limit_bytes=60 * 1024 * 1024
        ),
    )(
        inputs, segments, jnp.asarray(freqs), gains[0], w_query[0, 0], w_keyval[0, 0], w_output[0, 0]
    )
    return out[None]


def solution(mesh):
    return jax.shard_map(
        functools.partial(shards, mesh.shape["mesh"]),
        mesh=mesh,
        in_specs=(
            P("groups", None, "mesh"),
            P("groups", None),
            P("section", None, None),
            P("section", None, None, "mesh"),
            P("section", None, None, "mesh"),
            P("section", None, None, "mesh"),
        ),
        out_specs=P("section", "groups", None, "mesh"),
        check_vma=False,
    )
```

```python
import functools
import math

import jax
import jax.numpy as jnp
from jax import lax
from jax.experimental import pallas as pl
from jax.experimental.pallas import tpu as pltpu
from jax.sharding import PartitionSpec as P

HD = 128
GROUP = 8
CHUNKS = 2
norm_epsilon = 1e-05
rope_theta = 500000.0
MESH = pl.DeviceIdType.MESH
F32 = jnp.float32
BF16 = jnp.bfloat16


def inner_of(n):
    inner = 1
    while inner * 2 * inner * 2 <= n:
        inner *= 2
    return inner


def kernel(
    n,
    x_hbm,
    seg_ref,
    g_hbm,
    wq_hbm,
    wkv_hbm,
    wo_hbm,
    out_ref,
    xbuf,
    wq,
    wkv,
    wo,
    gbuf,
    ssq,
    kvbuf,
    att,
    fin,
    acc,
    acc_kv,
    scale_ref,
    cos_ref,
    sin_ref,
    mask_ref,
    in_sem,
    w_sem,
    w_send,
    x_recv,
    z_send,
    y_send,
    ssq_recv,
    ssq_send,
    kv_recv,
    kv_send,
    att_recv,
    att_send,
    out_send,
    out_recv,
    out_local,
):
    core = lax.axis_index("section")
    me = lax.axis_index("mesh")
    other = 1 - core
    inner = inner_of(n)
    outer = n // inner
    row, lane = me // inner, me % inner
    tok, cols = x_hbm.shape[1:]
    width = n * cols
    part = tok // CHUNKS
    first = me // GROUP * GROUP

    def block(layer, src):
        return xbuf.at[layer, :, pl.ds(pl.multiple_of(src * cols, cols), cols)]

    def send_to(src, dst, send, recv, peer):
        return pltpu.make_async_remote_copy(
            src_ref=src, dst_ref=dst, send_sem=send, recv_sem=recv,
            device_id={"mesh": peer}, device_id_type=MESH,
        )

    load_x = pltpu.make_async_copy(x_hbm.at[core], block(0, me), in_sem)
    load_x.start()
    weights = ((g_hbm, gbuf), (wq_hbm, wq), (wkv_hbm, wkv), (wo_hbm, wo))
    own_weights = [
        pltpu.make_async_copy(src, dst.at[core], w_sem.at[core, k]) for k, (src, dst) in enumerate(weights)
    ]
    sent_weights = [
        pltpu.make_async_remote_copy(
            src_ref=src, dst_ref=dst.at[core], send_sem=w_send.at[k], recv_sem=w_sem.at[core, k],
            device_id={"section": other}, device_id_type=MESH,
        )
        for k, (src, dst) in enumerate(weights)
    ]
    for copy in own_weights:
        copy.start()

    barrier = pltpu.get_barrier_semaphore()

    def greet(k, carry):
        pl.semaphore_signal(barrier, inc=1, device_id={"mesh": (me + k) % n}, device_id_type=MESH)
        return carry

    lax.fori_loop(1, n, greet, 0)
    pl.semaphore_signal(barrier, inc=1, device_id={"section": other}, device_id_type=MESH)
    load_x.wait()
    pl.semaphore_wait(barrier, n)

    def chunk(layer, c, src):
        return xbuf.at[layer, pl.ds(c * part, part), pl.ds(pl.multiple_of(src * cols, cols), cols)]

    def z_copy(layer, c, src, sign):
        return send_to(
            chunk(layer, c, src), chunk(layer, c, src), z_send.at[layer, c, (sign + 1) // 2, src // inner],
            x_recv.at[layer, c, src], me + sign * inner,
        )

    def y_copy(layer, c, src, k):
        return send_to(
            chunk(layer, c, src), chunk(layer, c, src), y_send.at[layer, c, k, src // inner],
            x_recv.at[layer, c, src], row * inner + (lane + k) % inner,
        )

    def arrived(layer, c, src):
        y_copy(layer, c, src, 0).wait_recv()

    def over_y(body):
        if inner == 2:
            body(1)
        else:
            def step(k, carry):
                body(k)
                return carry
            lax.fori_loop(1, inner, step, 0)

    def forward(layer, c, src, signs):
        for sign in signs:
            @pl.when((row + sign >= 0) & (row + sign < outer))
            def _():
                z_copy(layer, c, src, sign).start()
        over_y(lambda k: y_copy(layer, c, src, k).start())

    def over_peers(total, base, mine, body):
        def step(k, carry):
            body(base + (mine - base + k) % total)
            return carry
        lax.fori_loop(1, total, step, 0)

    def ssq_copy(layer, peer):
        return send_to(ssq.at[layer, me], ssq.at[layer, me], ssq_send.at[layer, peer], ssq_recv.at[layer, me], peer)

    def ssq_wait(layer, peer):
        send_to(ssq.at[layer, peer], ssq.at[layer, peer], ssq_send.at[layer, peer], ssq_recv.at[layer, peer], peer).wait_recv()

    def send_own(layer, value):
        floats = value.astype(F32)
        total = jnp.sum(floats * floats, axis=1, keepdims=True)
        ssq[layer, me] = jnp.transpose(jnp.broadcast_to(total, (tok, tok)))[:8]
        over_peers(n, 0, me, lambda peer: ssq_copy(layer, peer).start())
        for c in range(CHUNKS):
            forward(layer, c, me, (1, -1))

    send_own(0, block(0, me)[...])
    for copy in sent_weights:
        copy.start()

    seg = jnp.broadcast_to(seg_ref[pl.ds(core, 1), :].astype(F32), (tok, tok))
    t_index = lax.broadcasted_iota(jnp.int32, (tok, tok), 0)
    u_index = lax.broadcasted_iota(jnp.int32, (tok, tok), 1)
    allowed = jnp.where((seg == jnp.transpose(seg)) & (u_index <= t_index), 1.0, 0.0)
    mask_ref[...] = allowed
    positions = jnp.sum(allowed, axis=1, keepdims=True) - 1.0
    head_lane = lax.broadcasted_iota(jnp.int32, (tok, HD), 1)
    freqs = jnp.exp((head_lane % (HD // 2)).astype(F32) * (-2.0 * math.log(rope_theta) / HD))
    angles = positions * freqs
    cos_ref[...] = jnp.cos(angles)
    sine = jnp.sin(angles)
    sin_ref[...] = jnp.where(head_lane < HD // 2, -sine, sine)

    def rope(values):
        return (values * cos_ref[...] + pltpu.roll(values, HD // 2, 1) * sin_ref[...]).astype(BF16)

    def weight_wait(layer, k):
        src, dst = weights[k]
        pltpu.make_async_copy(src, dst.at[layer], w_sem.at[layer, k]).wait()

    def consume(layer, src):
        span = pl.ds(pl.multiple_of(src * cols, cols), cols)
        scale = jnp.concatenate([scale_ref[...]] * (cols // HD), axis=1)
        normed = (xbuf[layer, :, span].astype(F32) * scale * gbuf[layer, :, span].astype(F32)).astype(BF16)
        acc[...] += jnp.dot(normed, wq[layer, span, :], preferred_element_type=F32)
        acc_kv[...] += lax.dot_general(
            wkv[layer, :, span], normed, (((1,), (1,)), ((), ())), preferred_element_type=F32
        )

    for layer in range(2):
        over_peers(n, 0, me, lambda peer: ssq_wait(layer, peer))
        total = jnp.sum(ssq[layer], axis=0)
        scale_ref[...] = jnp.transpose(
            jnp.broadcast_to(lax.rsqrt(total[0:1, :] * (1.0 / width) + norm_epsilon), (HD, tok))
        )
        for k in range(3):
            weight_wait(layer, k)
        acc[...] = jnp.zeros_like(acc)
        acc_kv[...] = jnp.zeros_like(acc_kv)
        consume(layer, me)

        def side_blocks(distance):
            for sign in (1, -1):
                src_row = row - sign * distance

                @pl.when((src_row >= 0) & (src_row < outer))
                def _():
                    def take(k):
                        src = src_row * inner + (lane + k) % inner
                        for c in range(CHUNKS):
                            arrived(layer, c, src)
                        consume(layer, src)
                    over_y(take)

        def wave(distance, carry):
            for c in range(CHUNKS):
                for sign in (1, -1):
                    src_row = row - sign * distance

                    @pl.when((src_row >= 0) & (src_row < outer))
                    def _():
                        src = src_row * inner + lane
                        arrived(layer, c, src)
                        forward(layer, c, src, (sign,))
            for sign in (1, -1):
                src_row = row - sign * distance

                @pl.when((src_row >= 0) & (src_row < outer))
                def _():
                    consume(layer, src_row * inner + lane)

            @pl.when(distance > 1)
            def _():
                side_blocks(distance - 1)
            return carry

        def take_own_row(k):
            src = row * inner + (lane + k) % inner
            for c in range(CHUNKS):
                arrived(layer, c, src)
            consume(layer, src)

        lax.fori_loop(1, 2, wave, 0)
        over_y(take_own_row)
        lax.fori_loop(2, outer, wave, 0)
        side_blocks(outer - 1)

        kvbuf[layer, me - first] = acc_kv[...].astype(BF16)

        def kv_copy(peer):
            return send_to(
                kvbuf.at[layer, me - first], kvbuf.at[layer, me - first],
                kv_send.at[layer, peer - first], kv_recv.at[layer, me - first], peer,
            )

        def kv_wait(peer):
            send_to(
                kvbuf.at[layer, peer - first], kvbuf.at[layer, peer - first],
                kv_send.at[layer, peer - first], kv_recv.at[layer, peer - first], peer,
            ).wait_recv()

        over_peers(GROUP, first, me, lambda peer: kv_copy(peer).start())
        query = rope(acc[...])
        over_peers(GROUP, first, me, kv_wait)
        keyval = jnp.concatenate([kvbuf[layer, j] for j in range(GROUP)], axis=0)
        keys = rope(jnp.transpose(keyval[:HD].astype(F32)))
        scores = lax.dot_general(
            query, keys, (((1,), (1,)), ((), ())), preferred_element_type=F32
        ) * HD ** (-0.5)
        masked = jnp.where(mask_ref[...] > 0.0, scores, -1e30)
        raised = jnp.exp(masked - jnp.max(masked, axis=1, keepdims=True))
        probs = (raised / jnp.sum(raised, axis=1, keepdims=True)).astype(BF16)
        attended = lax.dot_general(
            probs, keyval[HD:], (((1,), (1,)), ((), ())), preferred_element_type=F32
        ).astype(BF16)

        def att_block(src):
            return att.at[layer, :, pl.ds(pl.multiple_of(src * HD, HD), HD)]

        def att_copy(peer):
            return send_to(att_block(me), att_block(me), att_send.at[layer, peer], att_recv.at[layer, me], peer)

        def att_wait(peer):
            send_to(att_block(peer), att_block(peer), att_send.at[layer, peer], att_recv.at[layer, peer], peer).wait_recv()

        att_block(me)[...] = attended
        over_peers(n, 0, me, lambda peer: att_copy(peer).start())
        weight_wait(layer, 3)
        over_peers(n, 0, me, att_wait)
        mixed = jnp.dot(att[layer], wo[layer], preferred_element_type=F32)
        result = (block(layer, me)[...].astype(F32) + mixed).astype(BF16)
        if layer == 0:
            block(1, me)[...] = result
            send_own(1, result)
            kept = block(1, me)
        else:
            fin[...] = result
            kept = fin

        @pl.when(core == layer)
        def _():
            pltpu.make_async_copy(kept, out_ref.at[core], out_local).start()

        @pl.when(core != layer)
        def _():
            pltpu.make_async_remote_copy(
                src_ref=kept, dst_ref=out_ref.at[core], send_sem=out_send, recv_sem=out_recv,
                device_id={"section": other}, device_id_type=MESH,
            ).start()

        over_peers(GROUP, first, me, lambda peer: kv_copy(peer).wait_send())
        over_peers(n, 0, me, lambda peer: att_copy(peer).wait_send())

    for layer in range(2):
        over_peers(n, 0, me, lambda peer: ssq_copy(layer, peer).wait_send())

        for c in range(CHUNKS):
            def drain(src_row, carry):
                src = src_row * inner + lane

                @pl.when((src_row <= row) & (row + 1 < outer))
                def _():
                    z_copy(layer, c, src, 1).wait_send()

                @pl.when((src_row >= row) & (row >= 1))
                def _():
                    z_copy(layer, c, src, -1).wait_send()

                over_y(lambda k: y_copy(layer, c, src, k).wait_send())
                return carry

            lax.fori_loop(0, outer, drain, 0)
    for copy in sent_weights:
        copy.wait_send()
    pltpu.make_async_copy(fin, out_ref.at[core], out_local).wait()
    last = pltpu.make_async_remote_copy(
        src_ref=fin, dst_ref=out_ref.at[other], send_sem=out_send, recv_sem=out_recv,
        device_id={"section": other}, device_id_type=MESH,
    )
    last.wait_send()
    last.wait_recv()


def shards(n, inputs, segments, gains, w_query, w_keyval, w_output):
    micro_count, tok, cols = inputs.shape
    width = gains.shape[-1]
    kvw = w_keyval.shape[-1]
    inner = inner_of(n)
    outer = n // inner
    dma = pltpu.SemaphoreType.DMA
    vmem = pl.BlockSpec(memory_space=pltpu.VMEM)
    hbm = pl.BlockSpec(memory_space=pl.ANY)
    out = pl.pallas_call(
        functools.partial(kernel, n),
        out_shape=jax.ShapeDtypeStruct((micro_count, tok, cols), BF16),
        in_specs=[hbm, vmem, hbm, hbm, hbm, hbm],
        out_specs=hbm,
        scratch_shapes=[
            pltpu.VMEM((2, tok, width), BF16),
            pltpu.VMEM((2, width, HD), BF16),
            pltpu.VMEM((2, kvw, width), BF16),
            pltpu.VMEM((2,) + w_output.shape[2:], BF16),
            pltpu.VMEM((2, 1, width), BF16),
            pltpu.VMEM((2, n, 8, tok), F32),
            pltpu.VMEM((2, GROUP, kvw, tok), BF16),
            pltpu.VMEM((2, tok, n * HD), BF16),
            pltpu.VMEM((tok, cols), BF16),
            pltpu.VMEM((tok, HD), F32),
            pltpu.VMEM((kvw, tok), F32),
            pltpu.VMEM((tok, HD), F32),
            pltpu.VMEM((tok, HD), F32),
            pltpu.VMEM((tok, HD), F32),
            pltpu.VMEM((tok, tok), F32),
            dma,
            dma((2, 4)),
            dma((4,)),
            dma((2, CHUNKS, n)),
            dma((2, CHUNKS, 2, outer)),
            dma((2, CHUNKS, max(inner, 2), outer)),
            dma((2, n)),
            dma((2, n)),
            dma((2, GROUP)),
            dma((2, GROUP)),
            dma((2, n)),
            dma((2, n)),
            dma,
            dma,
            dma,
        ],
        compiler_params=pltpu.CompilerParams(
            collective_id=0, has_side_effects=True, vmem_limit_bytes=60 * 1024 * 1024
        ),
    )(
        inputs, segments, gains[0], w_query[0, 0], jnp.swapaxes(w_keyval[0, 0], 0, 1), w_output[0, 0]
    )
    return out[None]


def solution(mesh):
    return jax.shard_map(
        functools.partial(shards, mesh.shape["mesh"]),
        mesh=mesh,
        in_specs=(
            P("groups", None, "mesh"),
            P("groups", None),
            P("section", None, None),
            P("section", None, None, "mesh"),
            P("section", None, None, "mesh"),
            P("section", None, None, "mesh"),
        ),
        out_specs=P("section", "groups", None, "mesh"),
        check_vma=False,
    )
```
